32 devices in a mesh: vocab: 4 (over z), dp: 8 (over y, x, core).
Axes of the slice: x: 2, y: 2, z: 4, core: 2. Of those that a mesh axis runs over, the one named last changes fastest.
Arguments:
- hidden: bfloat16 [2816, 4096], P('dp'), may hold values from -240 to 240
- output_projection_weight: bfloat16 [4096, 16384], P('dp', 'vocab'), may hold values from -0.25 to 0.25
- adapter_down_weight: bfloat16 [4096, 128], replicated, may hold values from -0.09375 to 0.09375
- adapter_up_weight: bfloat16 [128, 16384], P(None, 'vocab'), may hold values from -0.75 to 0.75
- labels: int32 [2816], P('dp'), may hold values from 0 to 16383
- token_job_index: int32 [2816], P('dp'), may hold values from 0 to 7, as said below
Outputs:
- logits: bfloat16 [2816, 16384], P('dp', 'vocab')
- logit_gradient_rows: bfloat16 [2816, 16384], P('dp', 'vocab')
- hidden_state_gradient: bfloat16 [2816, 4096], P('dp')
- token_loss: float32 [2816], P('dp')
- job_loss: float32 [8], replicated
The draws below stay inside these ranges and needn't reach their ends.
Inputs may be any that keep to these rules, and one draw needn't show every extreme that they name: `token_job_index`: a job may have no tokens at all, and the jobs' token counts differ widely.
All inputs are finite; a program needn't handle non-finite values.
Results may differ from the reference program's by a relative error of at most 0.014.
Values may be sent and summed in bfloat16 or wider, within the bound.
A program may use at most 256 MiB of HBM per device.

```python
import math
import jax
import jax.numpy as jnp
from jax import lax

MODEL_WIDTH = 4096
ADAPTER_JOBS = 8
ADAPTER_RANK = 16
TOKENS = 2816
VOCAB_ENTRIES = 16384


def draw_hidden(key, part):
    values = jnp.clip(jax.random.normal(key, (TOKENS, MODEL_WIDTH), jnp.float32), -6.0, 6.0)
    return values.astype(jnp.bfloat16)


def draw_token_job_index(key, part):
    order_key = jax.random.fold_in(key, 11)
    ticket_key = jax.random.fold_in(key, 12)
    order = jax.random.permutation(order_key, ADAPTER_JOBS).astype(jnp.int32)
    shares = [840 // (place + 1) for place in range(ADAPTER_JOBS - 1)] + [0]
    bounds_list = []
    running = 0
    for share in shares:
        running = running + share
        bounds_list.append(running)
    total_tickets = running
    bounds = jnp.array(bounds_list, dtype=jnp.int32)
    tickets = jax.random.randint(ticket_key, (TOKENS,), 0, total_tickets, dtype=jnp.int32)
    places = jnp.sum((tickets[:, None] >= bounds[None, :]).astype(jnp.int32), axis=1)
    return jnp.take(order, places).astype(jnp.int32)


def touch_ends(values, own_key, smallest, high):
    spot = [jax.random.randint(jax.random.fold_in(own_key, axis), (), 0, length) for axis, length in enumerate(values.shape)]
    main_axis = values.shape.index(max(values.shape))
    next_to = spot[:main_axis] + [(spot[main_axis] + 1) % values.shape[main_axis]] + spot[main_axis + 1:]
    return values.at[tuple(spot)].set(smallest).at[tuple(next_to)].set(high)


def shard_levels(own_key, extent, shards, smallest, high):
    gain, own = 1.0, jax.random.fold_in(own_key, 6)
    for dim, blocks in shards:
        draws = jnp.exp(jax.random.uniform(jax.random.fold_in(own, dim), (blocks,), jnp.float32, smallest / len(shards), high / len(shards)))
        gain = gain * jnp.repeat(draws, extent[dim] // blocks).reshape([-1 if axis == dim else 1 for axis in range(len(extent))])
    return gain


def bell_draw(rng, dims, width, bound, split=(), kind=jnp.bfloat16):
    level = shard_levels(rng, dims, split, -0.22, 0.18) if split else 1.0
    entries = jax.random.normal(rng, dims, jnp.float32) * width * level
    return jnp.minimum(jnp.maximum(entries, -bound), bound).astype(kind)


def setup_inputs(seed: int = 0) -> dict:
    key_list = jax.random.split(jax.random.key(seed), 7)
    return {
        "hidden": draw_hidden(jax.random.fold_in(key_list[6], 71), 0),
        "output_projection_weight": bell_draw(key_list[1], (MODEL_WIDTH, VOCAB_ENTRIES), (MODEL_WIDTH // 9) ** -0.5, 0.25, ((0, 8), (1, 4))),
        "adapter_down_weight": bell_draw(key_list[2], (MODEL_WIDTH, ADAPTER_JOBS * ADAPTER_RANK), MODEL_WIDTH ** -0.5, 0.09375),
        "adapter_up_weight": bell_draw(key_list[3], (ADAPTER_JOBS * ADAPTER_RANK, VOCAB_ENTRIES), (4 * ADAPTER_RANK) ** -0.5, 0.75, ((1, 4),)),
        "labels": touch_ends(jax.random.randint(key_list[4], (TOKENS,), 0, VOCAB_ENTRIES), jax.random.fold_in(key_list[4], 1), 0, VOCAB_ENTRIES - 1).astype(jnp.int32),
        "token_job_index": draw_token_job_index(jax.random.fold_in(key_list[6], 71), 0),
    }


def reference(hidden, output_projection_weight, adapter_down_weight, adapter_up_weight, labels, token_job_index):
    adapter_job_columns = ADAPTER_JOBS * ADAPTER_RANK
    col_job = lax.iota(jnp.int32, adapter_job_columns) // ADAPTER_RANK
    onehot = (token_job_index[:, None] == lax.iota(jnp.int32, ADAPTER_JOBS)[None, :]).astype(jnp.float32)
    counts = jnp.sum(onehot, axis=0)
    per_job = TOKENS / (ADAPTER_JOBS * jnp.maximum(counts, 1.0))
    block = math.gcd(TOKENS, 512)
    steps_count = TOKENS // block

    def one_block(index):
        start = (index * block).astype(jnp.int32)
        hidden_input = lax.dynamic_slice_in_dim(hidden, start, block, 0)
        lab = lax.dynamic_slice_in_dim(labels, start, block, 0)
        jid = lax.dynamic_slice_in_dim(token_job_index, start, block, 0)
        adapter_job_mask = (jid[:, None] == col_job[None, :]).astype(jnp.float32)
        adapter_input = (jnp.dot(hidden_input, adapter_down_weight, preferred_element_type=jnp.float32) * adapter_job_mask).astype(jnp.bfloat16)
        complete_logit_rows = jnp.dot(hidden_input, output_projection_weight, preferred_element_type=jnp.float32) + jnp.dot(adapter_input, adapter_up_weight, preferred_element_type=jnp.float32)
        row_max = jnp.max(complete_logit_rows, axis=1)
        shifted = jnp.exp(complete_logit_rows - row_max[:, None])
        exp_total = jnp.sum(shifted, axis=1)
        target_hit = lax.iota(jnp.int32, VOCAB_ENTRIES)[None, :] == lab[:, None]
        target = jnp.sum(jnp.where(target_hit, complete_logit_rows, 0.0), axis=1)
        token_loss = row_max + jnp.log(exp_total) - target
        token_weight = jnp.sum((jid[:, None] == lax.iota(jnp.int32, ADAPTER_JOBS)[None, :]).astype(jnp.float32) * per_job[None, :], axis=1)
        logit_gradient_rows = (token_weight[:, None] * (shifted / exp_total[:, None] - target_hit.astype(jnp.float32))).astype(jnp.bfloat16)
        adapter_gradient = jnp.dot(logit_gradient_rows, adapter_up_weight.T, preferred_element_type=jnp.float32)
        hidden_state_gradient = jnp.dot(logit_gradient_rows, output_projection_weight.T, preferred_element_type=jnp.float32) + jnp.dot(adapter_gradient * adapter_job_mask, adapter_down_weight.astype(jnp.float32).T, precision=lax.Precision.HIGHEST)
        return complete_logit_rows.astype(jnp.bfloat16), logit_gradient_rows, hidden_state_gradient.astype(jnp.bfloat16), token_loss

    logits, logit_gradient_rows, hidden_state_gradient, token_loss = lax.map(one_block, jnp.arange(steps_count, dtype=jnp.int32))
    logits = logits.reshape(TOKENS, VOCAB_ENTRIES)
    logit_gradient_rows = logit_gradient_rows.reshape(TOKENS, VOCAB_ENTRIES)
    hidden_state_gradient = hidden_state_gradient.reshape(TOKENS, MODEL_WIDTH)
    token_loss = token_loss.reshape(TOKENS)
    job_loss = jnp.sum(onehot * token_loss[:, None], axis=0) / jnp.maximum(counts, 1.0)
    return logits, logit_gradient_rows, hidden_state_gradient, token_loss, job_loss
```

```python
import functools
import math

import jax
import jax.numpy as jnp
from jax import lax
from jax.experimental import pallas as pl
from jax.experimental.pallas import tpu as pltpu
from jax.sharding import PartitionSpec as P

ADAPTER_JOBS = 8
ADAPTER_RANK = 16
MESH = pl.DeviceIdType.MESH
F32 = jnp.float32
BF16 = jnp.bfloat16
LAG_NEAR = 4
LAG_FAR = 7


def dot(a, b, dims=((1,), (0,))):
    return lax.dot_general(a, b, (dims, ((), ())), preferred_element_type=F32)


def kernel(
    n, v, tokens,
    hid, w_own, down, up, lab, job_col, job_row,
    logits_out, dl_out, dh_out, loss_out, job_out,
    w, acc, dl, stage, flow, stat_col, stat_mat, lora,
    cnt_own, cnt_in, job_own, job_in, st_own, st_in,
    own_sem, sq_send, sq_recv, low_send, low_recv,
    cnt_send, cnt_recv, job_send, job_recv, st_send, st_recv,
    flow_send, flow_recv, out_sem,
):
    rows = hid.shape[0]
    width, cols = w.shape
    block = w_own.shape[0]
    half = block // 2
    m = n // 4
    me = lax.axis_index("dp")
    vi = lax.axis_index("vocab")
    low = lax.rem(me, m)
    hi = me // m
    hx = lax.rem(hi, 2)
    hy = hi // 2
    xn = hy * 2 + (1 - hx)
    yn = (1 - hy) * 2 + hx
    dg = (1 - hy) * 2 + (1 - hx)
    row_block = math.gcd(rows, 32)
    col_tile = math.gcd(cols, 512)

    barrier = pltpu.get_barrier_semaphore()
    for k in range(1, n):
        pl.semaphore_signal(barrier, inc=1, device_id={"dp": lax.rem(me + k, n)}, device_id_type=MESH)
    for k in range(1, v):
        pl.semaphore_signal(barrier, inc=1, device_id={"vocab": lax.rem(vi + k, v)}, device_id_type=MESH)
    pl.semaphore_wait(barrier, n - 1 + v - 1)

    def place(h4, lo, h):
        start = pl.multiple_of((h4 * m + lo) * block + h * half, half)
        return w.at[pl.ds(start, half), :]

    def remote(src, dst, send, recv, **where):
        return pltpu.make_async_remote_copy(
            src_ref=src, dst_ref=dst, send_sem=send, recv_sem=recv,
            device_id=dict(where), device_id_type=MESH,
        )

    started = []

    def start(copy):
        copy.start()
        started.append(copy)

    def own(h):
        return w_own.at[pl.ds(h * half, half), :]

    for h in (1, 0):
        start(remote(own(h), place(hi, low, h), sq_send.at[h], sq_recv.at[h], dp=xn * m + low))
        g = 1 - h
        start(remote(own(g), place(hi, low, g), sq_send.at[2 + g], sq_recv.at[2 + g], dp=yn * m + low))

    def pass_low(slot, h4, h, src):
        for k in range(1, m):
            start(remote(
                src, place(h4, low, h), low_send.at[k - 1, slot], low_recv.at[k - 1, slot],
                dp=hi * m + lax.rem(low + k, m),
            ))

    pass_low(0, hi, 0, own(0))
    pass_low(1, hi, 1, own(1))
    local = [pltpu.make_async_copy(own(h), place(hi, low, h), own_sem.at[h]) for h in (0, 1)]
    for copy in local:
        copy.start()

    def landed(ref, sem):
        pltpu.make_async_copy(ref, ref, sem).wait()

    jobs = lax.broadcasted_iota(jnp.int32, (ADAPTER_JOBS, job_row.shape[1]), 0)
    onehot = (jobs == job_row[...]).astype(F32)
    cnt_own[...] = jnp.broadcast_to(jnp.sum(onehot, axis=1, keepdims=True), cnt_own.shape)

    rank_cols = down.shape[1]
    col_job = lax.broadcasted_iota(jnp.int32, (rows, rank_cols), 1) // ADAPTER_RANK
    mask = (job_col[...] == col_job).astype(F32)
    lora_in = (dot(hid[...], down[...]) * mask).astype(BF16)
    lora[...] = lora_in

    def seed(t, _):
        at = pl.ds(pl.multiple_of(t * col_tile, col_tile), col_tile)
        acc[:, at] = dot(lora[...], up[:, at])
        return 0

    lax.fori_loop(0, cols // col_tile, seed, 0)

    for k in range(1, n):
        start(remote(
            cnt_own, cnt_in.at[k - 1], cnt_send.at[k - 1], cnt_recv.at[k - 1], dp=lax.rem(me + k, n)
        ))

    def gain(h4, lo, h):
        first = pl.multiple_of((h4 * m + lo) * block + h * half, half)

        def tile(t, _):
            at = pl.ds(pl.multiple_of(t * col_tile, col_tile), col_tile)
            acc[:, at] += dot(hid[:, pl.ds(first, half)], w[pl.ds(first, half), at])
            return 0

        lax.fori_loop(0, cols // col_tile, tile, 0)

    def gain_low(slot, h4, h):
        for k in range(1, m):
            lo = lax.rem(low - k + m, m)
            landed(place(h4, lo, h), low_recv.at[k - 1, slot])
            gain(h4, lo, h)

    for h in (0, 1):
        local[h].wait()
        gain(hi, low, h)
    for h in (0, 1):
        gain_low(h, hi, h)

    landed(place(xn, low, 1), sq_recv.at[1])
    start(remote(place(xn, low, 1), place(xn, low, 1), sq_send.at[5], sq_recv.at[5], dp=yn * m + low))
    pass_low(2, xn, 1, place(xn, low, 1))
    landed(place(yn, low, 0), sq_recv.at[2])
    start(remote(place(yn, low, 0), place(yn, low, 0), sq_send.at[4], sq_recv.at[4], dp=xn * m + low))
    pass_low(3, yn, 0, place(yn, low, 0))
    gain(xn, low, 1)
    gain(yn, low, 0)
    gain_low(2, xn, 1)
    gain_low(3, yn, 0)
    landed(place(xn, low, 0), sq_recv.at[0])
    pass_low(4, xn, 0, place(xn, low, 0))
    landed(place(yn, low, 1), sq_recv.at[3])
    pass_low(5, yn, 1, place(yn, low, 1))
    gain(xn, low, 0)
    gain(yn, low, 1)
    gain_low(4, xn, 0)
    gain_low(5, yn, 1)
    landed(place(dg, low, 0), sq_recv.at[4])
    pass_low(6, dg, 0, place(dg, low, 0))
    landed(place(dg, low, 1), sq_recv.at[5])
    pass_low(7, dg, 1, place(dg, low, 1))
    gain(dg, low, 0)
    gain(dg, low, 1)
    gain_low(6, dg, 0)
    gain_low(7, dg, 1)

    col0 = vi * cols
    lane = lax.broadcasted_iota(jnp.int32, (row_block, 128), 1)
    stat_col[...] = jnp.zeros_like(stat_col)

    def stats(r, _):
        at = pl.ds(pl.multiple_of(r * row_block, row_block), row_block)
        x = acc[at, :]
        stage[at, :] = x.astype(BF16)
        top = jnp.max(x, axis=1, keepdims=True)
        total = jnp.sum(jnp.exp(x - top), axis=1, keepdims=True)
        hit = lax.broadcasted_iota(jnp.int32, x.shape, 1) == lab[at, :] - col0
        target = jnp.sum(jnp.where(hit, x, 0.0), axis=1, keepdims=True)
        stat_col[at, :] = jnp.where(
            lane == 0, top, jnp.where(lane == 1, total, jnp.where(lane == 2, target, 0.0))
        )
        return 0

    lax.fori_loop(0, rows // row_block, stats, 0)
    st_own[...] = stat_col[...].T[0:8, :]

    counts = cnt_own[...]
    for k in range(1, n):
        landed(cnt_in.at[k - 1], cnt_recv.at[k - 1])
        counts = counts + cnt_in[k - 1]
    counts = jnp.maximum(counts, 1.0)

    for k in range(1, v):
        start(remote(
            st_own, st_in.at[k - 1], st_send.at[k - 1], st_recv.at[k - 1], vocab=lax.rem(vi + k, v)
        ))
    logits_copy = pltpu.make_async_copy(stage, logits_out, out_sem.at[0])
    logits_copy.start()
    per_job = (tokens / ADAPTER_JOBS) / counts
    weight = jnp.sum(onehot * per_job[:, 0:1], axis=0, keepdims=True)

    top = st_own[0:1, :]
    total = st_own[1:2, :]
    target = st_own[2:3, :]
    for k in range(1, v):
        landed(st_in.at[k - 1], st_recv.at[k - 1])
        other = st_in[k - 1]
        joint = jnp.maximum(top, other[0:1, :])
        total = total * jnp.exp(top - joint) + other[1:2, :] * jnp.exp(other[0:1, :] - joint)
        target = target + other[2:3, :]
        top = joint
    real = lax.broadcasted_iota(jnp.int32, top.shape, 1) < rows
    total = jnp.where(real, total, 1.0)
    loss = jnp.where(real, top + jnp.log(total) - target, 0.0)
    loss_out[...] = jnp.broadcast_to(loss, loss_out.shape)
    job_own[...] = jnp.broadcast_to(jnp.sum(onehot * loss, axis=1, keepdims=True), job_own.shape)
    stat_mat[...] = jnp.zeros_like(stat_mat)
    stat_mat[0:1, :] = top
    stat_mat[1:2, :] = 1.0 / total
    stat_mat[2:3, :] = weight
    stat_col[...] = stat_mat[...].T

    def gradient(r, _):
        at = pl.ds(pl.multiple_of(r * row_block, row_block), row_block)
        x = acc[at, :]
        s = stat_col[at, :]
        hit = lax.broadcasted_iota(jnp.int32, x.shape, 1) == lab[at, :] - col0
        p = jnp.exp(x - s[:, 0:1]) * s[:, 1:2]
        dl[at, :] = (s[:, 2:3] * jnp.where(hit, p - 1.0, p)).astype(BF16)
        return 0

    lax.fori_loop(0, rows // row_block, gradient, 0)
    for k in range(1, n):
        start(remote(
            job_own, job_in.at[k - 1], job_send.at[k - 1], job_recv.at[k - 1], dp=lax.rem(me + k, n)
        ))
    dl_copy = pltpu.make_async_copy(dl, dl_out, out_sem.at[1])
    dl_copy.start()

    back = ((1,), (1,))
    g = dot(dl[...], up[...], back) * mask
    g0 = g.astype(BF16)
    g = g - g0.astype(F32)
    g1 = g.astype(BF16)
    g2 = (g - g1.astype(F32)).astype(BF16)
    lora[...] = g0
    logits_copy.wait()

    chunks = flow.shape[1]
    step = width // chunks
    near = vi // (v // 2)
    far = 1 - near
    near_to = lax.rem(vi + 1 - 2 * near + v, v)
    far_to = lax.rem(vi - 1 + 2 * near + v, v)
    is_end = jnp.logical_or(vi == 0, vi == v - 1)
    lag = jnp.where(is_end, 0, LAG_NEAR)

    def chunk_cols(c):
        return pl.ds(pl.multiple_of(c * step, step), step)

    def flow_copy(way, c, to):
        return remote(
            flow.at[way, c], flow.at[way, c], flow_send.at[way, c], flow_recv.at[way, c], vocab=to
        )

    def advance(s, _):
        @pl.when(s < chunks)
        def _():
            at = chunk_cols(s)
            d = down[at, :]
            acc[:, at] = (
                dot(dl[...], w[at, :], back) + dot(lora[...], d, back) + dot(g1, d, back) + dot(g2, d, back)
            )

        c = s - lag

        @pl.when(jnp.logical_and(c >= 0, c < chunks))
        def _():
            at = chunk_cols(c)

            @pl.when(is_end)
            def _():
                flow[near, c] = acc[:, at].astype(BF16)

            @pl.when(jnp.logical_not(is_end))
            def _():
                landed(flow.at[near, c], flow_recv.at[near, c])
                flow[near, c] = (flow[near, c].astype(F32) + acc[:, at]).astype(BF16)

            flow_copy(near, c, near_to).start()

        f = s - LAG_FAR

        @pl.when(f >= 0)
        def _():
            at = chunk_cols(f)
            landed(flow.at[far, f], flow_recv.at[far, f])
            came = flow[far, f].astype(F32)
            stage[:, at] = (came + flow[near, f].astype(F32)).astype(BF16)

            @pl.when(jnp.logical_not(is_end))
            def _():
                flow[far, f] = (came + acc[:, at]).astype(BF16)
                flow_copy(far, f, far_to).start()

        return 0

    lax.fori_loop(0, chunks + LAG_FAR, advance, 0)
    dh_copy = pltpu.make_async_copy(stage, dh_out, out_sem.at[2])
    dh_copy.start()

    sums = job_own[...]
    for k in range(1, n):
        landed(job_in.at[k - 1], job_recv.at[k - 1])
        sums = sums + job_in[k - 1]
    job_out[...] = sums / counts

    def drain(c, _):
        landed(flow.at[near, c], flow_send.at[near, c])

        @pl.when(jnp.logical_not(is_end))
        def _():
            landed(flow.at[far, c], flow_send.at[far, c])

        return 0

    lax.fori_loop(0, chunks, drain, 0)
    for copy in started:
        copy.wait_send()
    dl_copy.wait()
    dh_copy.wait()


def shards(n, v, hidden, w_own, down, up, labels, job_index):
    rows, width = hidden.shape
    cols = w_own.shape[1]
    padded = -(-rows // 128) * 128
    job_row = jnp.pad(job_index, (0, padded - rows), constant_values=-1)[None, :]
    chunks = 16
    dma = pltpu.SemaphoreType.DMA
    m = n // 4
    vmem = pl.BlockSpec(memory_space=pltpu.VMEM)
    hbm = pl.BlockSpec(memory_space=pl.ANY)
    logits, dl, dh, loss, job = pl.pallas_call(
        functools.partial(kernel, n, v, rows * n),
        out_shape=(
            jax.ShapeDtypeStruct((rows, cols), BF16),
            jax.ShapeDtypeStruct((rows, cols), BF16),
            jax.ShapeDtypeStruct((rows, width), BF16),
            jax.ShapeDtypeStruct((8, padded), F32),
            jax.ShapeDtypeStruct((ADAPTER_JOBS, 128), F32),
        ),
        in_specs=[vmem, hbm, vmem, vmem, vmem, vmem, vmem],
        out_specs=(hbm, hbm, hbm, vmem, vmem),
        scratch_shapes=[
            pltpu.VMEM((width, cols), BF16),
            pltpu.VMEM((rows, max(cols, width)), F32),
            pltpu.VMEM((rows, cols), BF16),
            pltpu.VMEM((rows, cols), BF16),
            pltpu.VMEM((2, chunks, rows, width // chunks), BF16),
            pltpu.VMEM((padded, 128), F32),
            pltpu.VMEM((128, padded), F32),
            pltpu.VMEM((rows, down.shape[1]), BF16),
            pltpu.VMEM((ADAPTER_JOBS, 128), F32),
            pltpu.VMEM((n - 1, ADAPTER_JOBS, 128), F32),
            pltpu.VMEM((ADAPTER_JOBS, 128), F32),
            pltpu.VMEM((n - 1, ADAPTER_JOBS, 128), F32),
            pltpu.VMEM((8, padded), F32),
            pltpu.VMEM((v - 1, 8, padded), F32),
            dma((2,)), dma((6,)), dma((6,)), dma((m - 1, 8)), dma((m - 1, 8)),
            dma((n - 1,)), dma((n - 1,)), dma((n - 1,)), dma((n - 1,)), dma((v - 1,)), dma((v - 1,)),
            dma((2, chunks)), dma((2, chunks)), dma((3,)),
        ],
        compiler_params=pltpu.CompilerParams(
            collective_id=0, has_side_effects=True, vmem_limit_bytes=66_000_000
        ),
    )(hidden, w_own, down, up, labels[:, None], job_index[:, None], job_row)
    return logits, dl, dh, loss[0, :rows], job[:, 0]


def solution(mesh):
    n, v = mesh.shape["dp"], mesh.shape["vocab"]
    in_specs = (P("dp", None), P("dp", "vocab"), P(), P(None, "vocab"), P("dp"), P("dp"))
    out_specs = (P("dp", "vocab"), P("dp", "vocab"), P("dp", None), P("dp"), P())
    return jax.shard_map(
        functools.partial(shards, n, v), mesh=mesh, in_specs=in_specs, out_specs=out_specs, check_vma=False
    )
```

```python
import functools
import math

import jax
import jax.numpy as jnp
from jax import lax
from jax.experimental import pallas as pl
from jax.experimental.pallas import tpu as pltpu
from jax.sharding import PartitionSpec as P

ADAPTER_JOBS = 8
ADAPTER_RANK = 16
MESH = pl.DeviceIdType.MESH
F32 = jnp.float32
BF16 = jnp.bfloat16
LAG_NEAR = 6
LAG_FAR = 11
PIECES = 4


def dot(a, b, dims=((1,), (0,))):
    return lax.dot_general(a, b, (dims, ((), ())), preferred_element_type=F32)


def kernel(
    n, v, tokens,
    hid, w_own, down, up, meta,
    logits_out, dl_out, dh_out, loss_out, job_out,
    w, acc, dl, stage, flow, stat_col, stat_mat, lab, lora,
    cnt_own, cnt_in, job_own, job_in, st_own, st_in,
    own_sem, sq_send, sq_recv, low_send, low_recv,
    cnt_send, cnt_recv, job_send, job_recv, st_send, st_recv,
    flow_send, flow_recv, out_sem,
):
    rows = hid.shape[0]
    width, cols = w.shape
    block = w_own.shape[0]
    half = block // 2
    piece = half // PIECES
    m = n // 4
    me = lax.axis_index("dp")
    vi = lax.axis_index("vocab")
    low = lax.rem(me, m)
    hi = me // m
    hx = lax.rem(hi, 2)
    hy = hi // 2
    xn = hy * 2 + (1 - hx)
    yn = (1 - hy) * 2 + hx
    dg = (1 - hy) * 2 + (1 - hx)
    row_block = math.gcd(rows, 32)
    col_tile = math.gcd(cols, 512)

    barrier = pltpu.get_barrier_semaphore()
    for k in range(1, n):
        pl.semaphore_signal(barrier, inc=1, device_id={"dp": lax.rem(me + k, n)}, device_id_type=MESH)
    for k in range(1, v):
        pl.semaphore_signal(barrier, inc=1, device_id={"vocab": lax.rem(vi + k, v)}, device_id_type=MESH)
    pl.semaphore_wait(barrier, n - 1 + v - 1)

    def rows_of(h4, lo, h, q=None):
        first = (h4 * m + lo) * block + h * half
        if q is None:
            return pl.ds(pl.multiple_of(first, half), half)
        return pl.ds(pl.multiple_of(first + q * piece, piece), piece)

    def place(h4, lo, h, q=None):
        return w.at[rows_of(h4, lo, h, q), :]

    def remote(src, dst, send, recv, **where):
        return pltpu.make_async_remote_copy(
            src_ref=src, dst_ref=dst, send_sem=send, recv_sem=recv,
            device_id=dict(where), device_id_type=MESH,
        )

    started = []

    def start(copy):
        copy.start()
        started.append(copy)

    def own(h):
        return w_own.at[pl.ds(h * half, half), :]

    for h in (1, 0):
        start(remote(own(h), place(hi, low, h), sq_send.at[h], sq_recv.at[h], dp=xn * m + low))
        g = 1 - h
        start(remote(own(g), place(hi, low, g), sq_send.at[2 + g], sq_recv.at[2 + g], dp=yn * m + low))

    def pass_low(slot, h4, h, src, q=None):
        for k in range(1, m):
            start(remote(
                src, place(h4, low, h, q), low_send.at[k - 1, slot], low_recv.at[k - 1, slot],
                dp=hi * m + lax.rem(low + k, m),
            ))

    pass_low(0, hi, 0, own(0))
    pass_low(1, hi, 1, own(1))
    local = [pltpu.make_async_copy(own(h), place(hi, low, h), own_sem.at[h]) for h in (0, 1)]
    for copy in local:
        copy.start()

    def landed(ref, sem):
        pltpu.make_async_copy(ref, ref, sem).wait()

    jobs = lax.broadcasted_iota(jnp.int32, (ADAPTER_JOBS, meta.shape[1]), 0)
    onehot = (jobs == meta[1:2, :]).astype(F32)
    cnt_own[...] = jnp.broadcast_to(jnp.sum(onehot, axis=1, keepdims=True), cnt_own.shape)

    stat_mat[...] = jnp.zeros_like(stat_mat)
    stat_mat[0:8, :] = meta[...].astype(F32)
    lab[...] = stat_mat[...].T.astype(jnp.int32)
    rank_cols = down.shape[1]
    col_job = lax.broadcasted_iota(jnp.int32, (rows, rank_cols), 1) // ADAPTER_RANK
    mask = (lab[0:rows, 1:2] == col_job).astype(F32)
    lora_in = (dot(hid[...], down[...]) * mask).astype(BF16)
    lora[...] = lora_in

    def seed(t, _):
        at = pl.ds(pl.multiple_of(t * col_tile, col_tile), col_tile)
        acc[:, at] = dot(lora[...], up[:, at])
        return 0

    lax.fori_loop(0, cols // col_tile, seed, 0)

    for k in range(1, n):
        start(remote(
            cnt_own, cnt_in.at[k - 1], cnt_send.at[k - 1], cnt_recv.at[k - 1], dp=lax.rem(me + k, n)
        ))

    groups = max(1, half // 128)
    per_group = PIECES // groups

    def gain(*parts):
        deeps = []
        for h4, lo, h, u in parts:
            size = half if u is None else half // groups
            first = (h4 * m + lo) * block + h * half + (0 if u is None else u * size)
            deeps.append(pl.ds(pl.multiple_of(first, size), size))

        def tile(t, _):
            at = pl.ds(pl.multiple_of(t * col_tile, col_tile), col_tile)
            more = acc[:, at]
            for deep in deeps:
                more += dot(hid[:, deep], w[deep, at])
            acc[:, at] = more
            return 0

        lax.fori_loop(0, cols // col_tile, tile, 0)

    def gain_low(*halves):
        for k in range(1, m):
            lo = lax.rem(low - k + m, m)
            for slot, h4, h in halves:
                landed(place(h4, lo, h), low_recv.at[k - 1, slot])
            gain(*[(h4, lo, h, None) for _, h4, h in halves])

    for copy in local:
        copy.wait()
    gain((hi, low, 0, None), (hi, low, 1, None))
    gain_low((0, hi, 0), (1, hi, 1))

    def relay(src4, h, first_slot, to):
        for q in range(PIECES):
            ref = place(src4, low, h, q)
            start(remote(ref, ref, sq_send.at[first_slot + q], sq_recv.at[first_slot + q], dp=to * m + low))

    landed(place(xn, low, 1), sq_recv.at[1])
    relay(xn, 1, 4 + PIECES, yn)
    pass_low(2, xn, 1, place(xn, low, 1))
    landed(place(yn, low, 0), sq_recv.at[2])
    relay(yn, 0, 4, xn)
    pass_low(3, yn, 0, place(yn, low, 0))
    gain((xn, low, 1, None), (yn, low, 0, None))
    gain_low((2, xn, 1), (3, yn, 0))
    landed(place(xn, low, 0), sq_recv.at[0])
    pass_low(4, xn, 0, place(xn, low, 0))
    landed(place(yn, low, 1), sq_recv.at[3])
    pass_low(5, yn, 1, place(yn, low, 1))
    gain((xn, low, 0, None), (yn, low, 1, None))
    gain_low((4, xn, 0), (5, yn, 1))
    for u in range(groups):
        mine = range(u * per_group, (u + 1) * per_group)
        for q in mine:
            for h in (0, 1):
                ref = place(dg, low, h, q)
                landed(ref, sq_recv.at[4 + h * PIECES + q])
                pass_low(6 + h * PIECES + q, dg, h, ref, q)
        gain((dg, low, 0, u), (dg, low, 1, u))
        for k in range(1, m):
            lo = lax.rem(low - k + m, m)
            for q in mine:
                for h in (0, 1):
                    landed(place(dg, lo, h, q), low_recv.at[k - 1, 6 + h * PIECES + q])
            gain((dg, lo, 0, u), (dg, lo, 1, u))

    col0 = vi * cols
    lane = lax.broadcasted_iota(jnp.int32, (row_block, 128), 1)
    stat_col[...] = jnp.zeros_like(stat_col)

    def stats(r, _):
        at = pl.ds(pl.multiple_of(r * row_block, row_block), row_block)
        x = acc[at, :]
        stage[at, :] = x.astype(BF16)
        top = jnp.max(x, axis=1, keepdims=True)
        total = jnp.sum(jnp.exp(x - top), axis=1, keepdims=True)
        hit = lax.broadcasted_iota(jnp.int32, x.shape, 1) == lab[at, 0:1] - col0
        target = jnp.sum(jnp.where(hit, x, 0.0), axis=1, keepdims=True)
        stat_col[at, :] = jnp.where(
            lane == 0, top, jnp.where(lane == 1, total, jnp.where(lane == 2, target, 0.0))
        )
        return 0

    lax.fori_loop(0, rows // row_block, stats, 0)
    st_own[...] = stat_col[...].T[0:8, :]

    counts = cnt_own[...]
    for k in range(1, n):
        landed(cnt_in.at[k - 1], cnt_recv.at[k - 1])
        counts = counts + cnt_in[k - 1]
    counts = jnp.maximum(counts, 1.0)

    for k in range(1, v):
        start(remote(
            st_own, st_in.at[k - 1], st_send.at[k - 1], st_recv.at[k - 1], vocab=lax.rem(vi + k, v)
        ))
    logits_copy = pltpu.make_async_copy(stage, logits_out, out_sem.at[0])
    logits_copy.start()
    per_job = (tokens / ADAPTER_JOBS) / counts
    weight = jnp.sum(onehot * per_job[:, 0:1], axis=0, keepdims=True)

    top = st_own[0:1, :]
    total = st_own[1:2, :]
    target = st_own[2:3, :]
    for k in range(1, v):
        landed(st_in.at[k - 1], st_recv.at[k - 1])
        other = st_in[k - 1]
        joint = jnp.maximum(top, other[0:1, :])
        total = total * jnp.exp(top - joint) + other[1:2, :] * jnp.exp(other[0:1, :] - joint)
        target = target + other[2:3, :]
        top = joint
    real = lax.broadcasted_iota(jnp.int32, top.shape, 1) < rows
    total = jnp.where(real, total, 1.0)
    loss = jnp.where(real, top + jnp.log(total) - target, 0.0)
    loss_out[...] = jnp.broadcast_to(loss, loss_out.shape)
    job_own[...] = jnp.broadcast_to(jnp.sum(onehot * loss, axis=1, keepdims=True), job_own.shape)
    stat_mat[...] = jnp.zeros_like(stat_mat)
    stat_mat[0:1, :] = top
    stat_mat[1:2, :] = 1.0 / total
    stat_mat[2:3, :] = weight
    stat_col[...] = stat_mat[...].T

    def gradient(r, _):
        at = pl.ds(pl.multiple_of(r * row_block, row_block), row_block)
        x = acc[at, :]
        s = stat_col[at, :]
        hit = lax.broadcasted_iota(jnp.int32, x.shape, 1) == lab[at, 0:1] - col0
        p = jnp.exp(x - s[:, 0:1]) * s[:, 1:2]
        dl[at, :] = (s[:, 2:3] * jnp.where(hit, p - 1.0, p)).astype(BF16)
        return 0

    lax.fori_loop(0, rows // row_block, gradient, 0)
    for k in range(1, n):
        start(remote(
            job_own, job_in.at[k - 1], job_send.at[k - 1], job_recv.at[k - 1], dp=lax.rem(me + k, n)
        ))
    dl_copy = pltpu.make_async_copy(dl, dl_out, out_sem.at[1])
    dl_copy.start()

    back = ((1,), (1,))
    g = dot(dl[...], up[...], back) * mask
    g0 = g.astype(BF16)
    g = g - g0.astype(F32)
    g1 = g.astype(BF16)
    g2 = (g - g1.astype(F32)).astype(BF16)
    lora[...] = g0
    logits_copy.wait()

    chunks = flow.shape[1]
    step = width // chunks
    near = vi // (v // 2)
    far = 1 - near
    near_to = lax.rem(vi + 1 - 2 * near + v, v)
    far_to = lax.rem(vi - 1 + 2 * near + v, v)
    is_end = jnp.logical_or(vi == 0, vi == v - 1)
    lag = jnp.where(is_end, 0, LAG_NEAR)

    def chunk_cols(c):
        return pl.ds(pl.multiple_of(c * step, step), step)

    def flow_copy(way, c, to):
        return remote(
            flow.at[way, c], flow.at[way, c], flow_send.at[way, c], flow_recv.at[way, c], vocab=to
        )

    def advance(multiply, s, _):
        if multiply:
            at = chunk_cols(s)
            d = down[at, :]
            acc[:, at] = (
                dot(dl[...], w[at, :], back) + dot(lora[...], d, back) + dot(g1, d, back) + dot(g2, d, back)
            )

        c = s - lag

        @pl.when(jnp.logical_and(c >= 0, c < chunks))
        def _():
            at = chunk_cols(c)

            @pl.when(is_end)
            def _():
                flow[near, c] = acc[:, at].astype(BF16)

            @pl.when(jnp.logical_not(is_end))
            def _():
                landed(flow.at[near, c], flow_recv.at[near, c])
                flow[near, c] = (flow[near, c].astype(F32) + acc[:, at]).astype(BF16)

            flow_copy(near, c, near_to).start()

        f = s - LAG_FAR

        @pl.when(f >= 0)
        def _():
            at = chunk_cols(f)
            landed(flow.at[far, f], flow_recv.at[far, f])
            came = flow[far, f].astype(F32)
            stage[:, at] = (came + flow[near, f].astype(F32)).astype(BF16)

            @pl.when(jnp.logical_not(is_end))
            def _():
                flow[far, f] = (came + acc[:, at]).astype(BF16)
                flow_copy(far, f, far_to).start()

        return 0

    lax.fori_loop(0, chunks, functools.partial(advance, True), 0)
    ready = (chunks - LAG_FAR) * step
    dh_copies = [
        pltpu.make_async_copy(stage.at[:, part], dh_out.at[:, part], out_sem.at[2 + k])
        for k, part in enumerate((pl.ds(0, ready), pl.ds(ready, width - ready)))
    ]
    dh_copies[0].start()
    lax.fori_loop(chunks, chunks + LAG_FAR, functools.partial(advance, False), 0)
    dh_copies[1].start()

    sums = job_own[...]
    for k in range(1, n):
        landed(job_in.at[k - 1], job_recv.at[k - 1])
        sums = sums + job_in[k - 1]
    job_out[...] = sums / counts

    def drain(c, _):
        landed(flow.at[near, c], flow_send.at[near, c])

        @pl.when(jnp.logical_not(is_end))
        def _():
            landed(flow.at[far, c], flow_send.at[far, c])

        return 0

    lax.fori_loop(0, chunks, drain, 0)
    for copy in started:
        copy.wait_send()
    dl_copy.wait()
    for copy in dh_copies:
        copy.wait()


def shards(n, v, hidden, w_own, down, up, labels, job_index):
    rows, width = hidden.shape
    cols = w_own.shape[1]
    padded = -(-rows // 128) * 128
    tail = ((0, 6), (0, padded - rows))
    meta = jnp.pad(jnp.stack([labels, job_index]), tail, constant_values=-1)
    chunks = 32
    dma = pltpu.SemaphoreType.DMA
    m = n // 4
    vmem = pl.BlockSpec(memory_space=pltpu.VMEM)
    hbm = pl.BlockSpec(memory_space=pl.ANY)
    logits, dl, dh, loss, job = pl.pallas_call(
        functools.partial(kernel, n, v, rows * n),
        out_shape=(
            jax.ShapeDtypeStruct((rows, cols), BF16),
            jax.ShapeDtypeStruct((rows, cols), BF16),
            jax.ShapeDtypeStruct((rows, width), BF16),
            jax.ShapeDtypeStruct((8, padded), F32),
            jax.ShapeDtypeStruct((ADAPTER_JOBS, 128), F32),
        ),
        in_specs=[vmem, hbm, vmem, vmem, vmem],
        out_specs=(hbm, hbm, hbm, vmem, vmem),
        scratch_shapes=[
            pltpu.VMEM((width, cols), BF16),
            pltpu.VMEM((rows, max(cols, width)), F32),
            pltpu.VMEM((rows, cols), BF16),
            pltpu.VMEM((rows, cols), BF16),
            pltpu.VMEM((2, chunks, rows, width // chunks), BF16),
            pltpu.VMEM((padded, 128), F32),
            pltpu.VMEM((128, padded), F32),
            pltpu.VMEM((padded, 128), jnp.int32),
            pltpu.VMEM((rows, down.shape[1]), BF16),
            pltpu.VMEM((ADAPTER_JOBS, 128), F32),
            pltpu.VMEM((n - 1, ADAPTER_JOBS, 128), F32),
            pltpu.VMEM((ADAPTER_JOBS, 128), F32),
            pltpu.VMEM((n - 1, ADAPTER_JOBS, 128), F32),
            pltpu.VMEM((8, padded), F32),
            pltpu.VMEM((v - 1, 8, padded), F32),
            dma((2,)), dma((4 + 2 * PIECES,)), dma((4 + 2 * PIECES,)),
            dma((m - 1, 6 + 2 * PIECES)), dma((m - 1, 6 + 2 * PIECES)),
            dma((n - 1,)), dma((n - 1,)), dma((n - 1,)), dma((n - 1,)), dma((v - 1,)), dma((v - 1,)),
            dma((2, chunks)), dma((2, chunks)), dma((4,)),
        ],
        compiler_params=pltpu.CompilerParams(
            collective_id=0, has_side_effects=True, vmem_limit_bytes=66_000_000
        ),
    )(hidden, w_own, down, up, meta)
    return logits, dl, dh, loss[0, :rows], job[:, 0]


def solution(mesh):
    n, v = mesh.shape["dp"], mesh.shape["vocab"]
    in_specs = (P("dp", None), P("dp", "vocab"), P(), P(None, "vocab"), P("dp"), P("dp"))
    out_specs = (P("dp", "vocab"), P("dp", "vocab"), P("dp", None), P("dp"), P())
    return jax.shard_map(
        functools.partial(shards, n, v), mesh=mesh, in_specs=in_specs, out_specs=out_specs, check_vma=False
    )
```
